32 devices in a mesh: lon: 8 (over z, y), day: 4 (over x, core).
Axes of the slice: x: 2, y: 2, z: 4, core: 2. Of those that a mesh axis runs over, the one named last changes fastest.
Arguments:
- field: bfloat16 [92, 720, 1024], P('day', 'lon'), may hold values from -6 to 6
Outputs:
- filtered: float32 [92, 720, 1024], P('day', 'lon')
The draws below stay inside these ranges and needn't reach their ends.
All inputs are finite; a program needn't handle non-finite values.
Results may differ from the reference program's by a relative error of at most 0.0003.
Values may be sent and summed in bfloat16 or wider, within the bound.
A program may use at most 192 MiB of HBM per device.

```python
import jax
import jax.numpy as jnp
from jax import lax

COLS = 1024
LON = 720
DAYS = 92
DAY_HALF = 15
LON_HALF = 10


def levels(stream_key, extent, cuts, least, top_value):
    def one(position, shards_of):
        draws = jax.random.uniform(jax.random.fold_in(jax.random.fold_in(stream_key, 6), position), (shards_of,), jnp.float32, least / len(cuts), top_value / len(cuts))
        return jnp.repeat(jnp.exp(draws), extent[position] // shards_of).reshape((-1,) + (1,) * (len(extent) - position - 1))

    level = one(*cuts[0])
    for cut in cuts[1:]:
        level = level * one(*cut)
    return level


def centred(stream_key, dims, deviation, reach, shards=(), kind=jnp.bfloat16):
    drawn = jax.random.normal(stream_key, dims, jnp.float32) * deviation
    if len(shards) > 0:
        drawn = levels(stream_key, dims, shards, -0.22, 0.18) * drawn
    return jnp.clip(drawn, min=-reach, max=reach).astype(kind)


def setup_inputs(seed: int = 0) -> dict:
    key_list = jax.random.split(jax.random.key(seed), 2)
    field = centred(key_list[0], (DAYS, LON, COLS), 1.0, 6.0, ((0, 4), (1, 8)))
    return {"field": field}


def running(values, dim, half):
    count = values.shape[dim] - 2 * half
    total = jnp.cumsum(values, axis=dim)
    first = jnp.zeros_like(lax.slice_in_dim(total, 0, 1, axis=dim))
    total = jnp.concatenate([first, total], axis=dim)
    upper = lax.slice_in_dim(total, 2 * half + 1, 2 * half + 1 + count, axis=dim)
    lower = lax.slice_in_dim(total, 0, count, axis=dim)
    return (upper - lower) / (2.0 * half + 1.0)


def wrapped(values, dim, half):
    size = values.shape[dim]
    head = lax.slice_in_dim(values, size - half, size, axis=dim)
    tail = lax.slice_in_dim(values, 0, half, axis=dim)
    return jnp.concatenate([head, values, tail], axis=dim)


def one_block(block):
    values = block.astype(jnp.float32)
    clim = running(wrapped(values, 0, DAY_HALF), 0, DAY_HALF)
    anomaly = values - clim
    return running(wrapped(anomaly, 1, LON_HALF), 1, LON_HALF)


def reference(field):
    width = 128 if COLS % 128 == 0 else COLS
    blocks = COLS // width
    split = field.reshape(DAYS, LON, blocks, width)
    split = jnp.moveaxis(split, 2, 0)
    result = lax.map(one_block, split)
    return jnp.moveaxis(result, 0, 2).reshape(DAYS, LON, COLS)
```

```python
import functools

import jax
import jax.numpy as jnp
from jax import lax
from jax.experimental import pallas as pl
from jax.experimental.pallas import tpu as pltpu
from jax.sharding import PartitionSpec as P

DAY_HALF = 15
LON_HALF = 10
ROWS = 8
MESH = pl.DeviceIdType.MESH


def pieces(lo, hi, size):
    return [(at, min(size, hi - at)) for at in range(lo, hi, size)]


def plan(lons):
    half = LON_HALF
    left = pieces(0, half, half // 2)
    right = pieces(lons - half, lons, half // 2)
    edges = [piece for pair in zip(left, right) for piece in pair]
    middle = pieces(half, lons - half, half)
    at, size = middle.pop()
    middle += pieces(at, at + size, half // 2)
    return edges, middle


def band(days, rows, shift):
    day = lax.broadcasted_iota(jnp.int32, (days, rows), 0)
    other = lax.broadcasted_iota(jnp.int32, (days, rows), 1) + shift
    away = jnp.abs(day - other)
    weight = jnp.where(away <= DAY_HALF, -1.0, 0.0)
    if shift == 0:
        weight = jnp.where(away == 0, 2.0 * DAY_HALF, weight)
    return weight.astype(jnp.bfloat16)


def kernel(
    counts, x, out, own, before, after, anomaly,
    own_sem, day_send, day_recv, lon_send, lon_recv,
):
    lons, days, cols = x.shape
    half = LON_HALF
    tail = days - before.shape[1]
    head = after.shape[1]
    day_count, lon_count = counts
    day, lon = lax.axis_index("day"), lax.axis_index("lon")
    day_next = lax.rem(day + 1, day_count)
    day_back = lax.rem(day + day_count - 1, day_count)
    lon_next = lax.rem(lon + 1, lon_count)
    lon_back = lax.rem(lon + lon_count - 1, lon_count)
    edges, middle = plan(lons)
    order = edges + middle

    loads = []
    for n, (at, size) in enumerate(order):
        loads.append(
            pltpu.make_async_copy(
                x.at[pl.ds(at, size)], own.at[pl.ds(at, size)], own_sem.at[n]
            )
        )
        loads[-1].start()

    barrier = pltpu.get_barrier_semaphore()
    for axis, peer in (
        ("day", day_next), ("day", day_back), ("lon", lon_next), ("lon", lon_back),
    ):
        pl.semaphore_signal(
            barrier, inc=1, device_id={axis: peer}, device_id_type=MESH
        )
    pl.semaphore_wait(barrier, 4)

    swaps = []
    for n, (at, size) in enumerate(order):
        up = pltpu.make_async_remote_copy(
            src_ref=x.at[pl.ds(at, size), pl.ds(tail, days - tail)],
            dst_ref=before.at[pl.ds(at, size)],
            send_sem=day_send.at[0, n],
            recv_sem=day_recv.at[0, n],
            device_id={"day": day_next},
            device_id_type=MESH,
        )
        down = pltpu.make_async_remote_copy(
            src_ref=x.at[pl.ds(at, size), pl.ds(0, head)],
            dst_ref=after.at[pl.ds(at, size)],
            send_sem=day_send.at[1, n],
            recv_sem=day_recv.at[1, n],
            device_id={"day": day_back},
            device_id_type=MESH,
        )
        up.start()
        down.start()
        swaps.append((up, down))

    own_band = band(days, days, 0)
    before_band = band(days, days - tail, tail - days)
    after_band = band(days, head, days)

    def dot(weight, values):
        return jnp.dot(weight, values, preferred_element_type=jnp.float32)

    def daily(n):
        at, size = order[n]
        loads[n].wait()
        for copy in swaps[n]:
            copy.wait_recv()

        @pl.loop(at, at + size)
        def _(l):
            anomaly[l + half] = (
                dot(own_band, own[l])
                + dot(before_band, before[l])
                + dot(after_band, after[l])
            )

    def edge(n):
        at, size = order[n]
        low = at < half
        place = at + lons + half if low else at - lons + half
        side = 0 if low else 1
        copy = pltpu.make_async_remote_copy(
            src_ref=anomaly.at[pl.ds(at + half, size)],
            dst_ref=anomaly.at[pl.ds(place, size)],
            send_sem=lon_send.at[side, n],
            recv_sem=lon_recv.at[side, n],
            device_id={"lon": lon_back if low else lon_next},
            device_id_type=MESH,
        )
        copy.start()
        return copy

    shifts = []
    for n in range(len(edges)):
        daily(n)
        shifts.append(edge(n))

    scale = 1.0 / ((2 * DAY_HALF + 1) * (2 * half + 1))
    width = 2 * half + 1

    def up_to(lo, hi, total):
        def step(l, total):
            total = total + (anomaly[l + width - 1] - anomaly[l - 1])
            out[l] = total * scale
            return total

        return lax.fori_loop(lo, hi, step, total)

    total = None
    done = half
    for n in range(len(edges), len(order)):
        daily(n)
        ready = sum(order[n]) - half
        if n == len(order) - 1:
            ready = lons - half
        if ready <= half:
            continue
        if total is None:
            total = lax.fori_loop(
                half, half + width, lambda l, t: t + anomaly[l], jnp.zeros((days, cols), jnp.float32)
            )
            out[half] = total * scale
            first = total
            done = half + 1
        total = up_to(done, ready, total)
        done = ready
    for copy in shifts:
        copy.wait_recv()
    up_to(done, lons, total)

    def back(step, total):
        l = half - 1 - step
        total = total + (anomaly[l] - anomaly[l + width])
        out[l] = total * scale
        return total

    lax.fori_loop(0, half, back, first)

    for pair in swaps:
        for copy in pair:
            copy.wait_send()
    for copy in shifts:
        copy.wait_send()


def local(counts, field):
    days, lons, cols = field.shape
    x = jnp.transpose(field, (1, 0, 2))
    tail = (days - DAY_HALF) // ROWS * ROWS
    head = min(days, (DAY_HALF + ROWS - 1) // ROWS * ROWS)
    edges, middle = plan(lons)
    steps = len(edges) + len(middle)
    y = pl.pallas_call(
        functools.partial(kernel, counts),
        out_shape=pltpu.VMEM((lons, days, cols), jnp.float32),
        in_specs=[pl.BlockSpec(memory_space=pltpu.HBM)],
        out_specs=pl.BlockSpec(memory_space=pltpu.VMEM),
        scratch_shapes=[
            pltpu.VMEM((lons, days, cols), jnp.bfloat16),
            pltpu.VMEM((lons, days - tail, cols), jnp.bfloat16),
            pltpu.VMEM((lons, head, cols), jnp.bfloat16),
            pltpu.VMEM((lons + 2 * LON_HALF, days, cols), jnp.float32),
            pltpu.SemaphoreType.DMA((steps,)),
            pltpu.SemaphoreType.DMA((2, steps)),
            pltpu.SemaphoreType.DMA((2, steps)),
            pltpu.SemaphoreType.DMA((2, len(edges))),
            pltpu.SemaphoreType.DMA((2, len(edges))),
        ],
        compiler_params=pltpu.CompilerParams(
            collective_id=0, has_side_effects=True, vmem_limit_bytes=50 * 1024 * 1024
        ),
    )(x)
    return jnp.transpose(y, (1, 0, 2))


def solution(mesh):
    return jax.shard_map(
        functools.partial(local, (mesh.shape["day"], mesh.shape["lon"])),
        mesh=mesh,
        in_specs=(P("day", "lon", None),),
        out_specs=P("day", "lon", None),
        check_vma=False,
    )
```

```python
import functools

import jax
import jax.numpy as jnp
from jax import lax
from jax.experimental import pallas as pl
from jax.experimental.pallas import tpu as pltpu
from jax.sharding import PartitionSpec as P

DAY_HALF = 15
LON_HALF = 10
ROWS = 8
PAD = 24
LEAD = 3
MESH = pl.DeviceIdType.MESH


def plan(lons):
    group = DAY_HALF % ROWS + 1
    depth = -(-LON_HALF // group) * group
    left = [(at, group) for at in range(0, depth, group)]
    right = [(lons - at - group, group) for at in range(0, depth, group)]
    edges = [piece for pair in zip(left, right) for piece in pair]
    middle = [
        (at, min(group, lons - depth - at)) for at in range(depth, lons - depth, group)
    ]
    return edges, middle


def grid(rows, cols):
    return (
        lax.broadcasted_iota(jnp.int32, (rows, cols), 0),
        lax.broadcasted_iota(jnp.int32, (rows, cols), 1),
    )


def ones(condition):
    return jnp.where(condition, 1.0, 0.0).astype(jnp.bfloat16)


def band(days, rows, shift):
    day, other = grid(days, rows)
    away = jnp.abs(day - other - shift)
    weight = jnp.where(away <= DAY_HALF, -1.0, 0.0)
    if shift == 0:
        weight = jnp.where(away == 0, 2.0 * DAY_HALF, weight)
    return weight.astype(jnp.bfloat16)


def stacked(days, shift, extra):
    row, other = grid(2 * PAD, 2 * ROWS)
    low = (row < days) & (other < DAY_HALF) & (jnp.abs(row - other - shift) <= DAY_HALF)
    away = jnp.abs(row - PAD - (ROWS + extra) - shift)
    high = (row >= PAD) & (row < PAD + days) & (other == DAY_HALF) & (away <= DAY_HALF)
    return jnp.where(low | high, -1.0, 0.0).astype(jnp.bfloat16)


def kernel(
    counts, x, out, own, before, after, rest_before, rest_after, pack_up, pack_down,
    anomaly, own_sem, day_send, day_recv, lon_send, lon_recv,
):
    lons, days, cols = x.shape
    half = LON_HALF
    tail = days - DAY_HALF
    part = DAY_HALF - ROWS
    group = part + 1
    day_count, lon_count = counts
    day, lon = lax.axis_index("day"), lax.axis_index("lon")
    day_next = lax.rem(day + 1, day_count)
    day_back = lax.rem(day + day_count - 1, day_count)
    lon_next = lax.rem(lon + 1, lon_count)
    lon_back = lax.rem(lon + lon_count - 1, lon_count)
    edges, middle = plan(lons)
    order = edges + middle

    loads = []
    for n, (at, size) in enumerate(order):
        loads.append(
            pltpu.make_async_copy(
                x.at[pl.ds(at, size)], own.at[pl.ds(at, size)], own_sem.at[n]
            )
        )
        loads[-1].start()

    barrier = pltpu.get_barrier_semaphore()
    for axis, peer in (
        ("day", day_next), ("day", day_back), ("lon", lon_next), ("lon", lon_back),
    ):
        pl.semaphore_signal(
            barrier, inc=1, device_id={axis: peer}, device_id_type=MESH
        )
    pl.semaphore_wait(barrier, 4)

    swaps = [[] for _ in order]

    def swap(n, kind, up_src, up_dst, down_src, down_dst):
        for way, src, dst, peer in (
            (0, up_src, up_dst, day_next), (1, down_src, down_dst, day_back),
        ):
            copy = pltpu.make_async_remote_copy(
                src_ref=src,
                dst_ref=dst,
                send_sem=day_send.at[kind, way, n],
                recv_sem=day_recv.at[kind, way, n],
                device_id={"day": peer},
                device_id_type=MESH,
            )
            copy.start()
            swaps[n].append(copy)

    def whole(n):
        at, size = order[n]
        if size == group:
            rows = pl.ds(at, size)
            swap(
                n, 0,
                x.at[rows, pl.ds(tail, ROWS)], before.at[rows, pl.ds(0, ROWS)],
                x.at[rows, pl.ds(0, ROWS)], after.at[rows, pl.ds(0, ROWS)],
            )
        else:
            rows = pl.ds(at, size)
            swap(
                n, 0,
                x.at[rows, pl.ds(tail, DAY_HALF)], rest_before,
                x.at[rows, pl.ds(0, 2 * ROWS)], rest_after,
            )

    row, col = grid(2 * ROWS, days)
    first_day = jnp.where(row < ROWS, tail + ROWS, ROWS)
    place = jnp.where(row < ROWS, row, row - ROWS)
    keep = ones((place < part) & (col == first_day + place))

    def dot(weight, values):
        return jnp.dot(weight, values, preferred_element_type=jnp.float32)

    def pack(n):
        at, size = order[n]
        loads[n].wait()
        if size < group:
            return

        @pl.loop(0, part)
        def _(i):
            ride = ones((place == part) & (col == first_day + i))
            tile = dot(keep, own[at + i]) + dot(ride, own[at + part])
            tile = tile.astype(jnp.bfloat16)
            pack_up[at + i] = tile[:ROWS]
            pack_down[at + i] = tile[ROWS:]

    def packed(n):
        at, size = order[n]
        if size == group:
            rows = pl.ds(at, part)
            swap(
                n, 1,
                pack_up.at[rows], before.at[rows, pl.ds(ROWS, ROWS)],
                pack_down.at[rows], after.at[rows, pl.ds(ROWS, ROWS)],
            )

    own_band = band(days, days, 0)
    before_band = band(days, DAY_HALF, -DAY_HALF)
    after_band = band(days, 2 * ROWS, days)
    before_top = band(days, ROWS, -DAY_HALF)
    after_top = band(days, ROWS, days)

    def daily(n):
        at, size = order[n]
        for copy in swaps[n]:
            copy.wait_recv()
        if size < group:
            for i in range(size):
                anomaly[at + i + half] = (
                    dot(own_band, own[at + i])
                    + dot(before_band, rest_before[i])
                    + dot(after_band, rest_after[i])
                )
            return

        last = at + part
        anomaly[last + half] = (
            dot(own_band, own[last])
            + dot(before_top, before[last, pl.ds(0, ROWS)])
            + dot(after_top, after[last, pl.ds(0, ROWS)])
        )

        @pl.loop(0, part)
        def _(i):
            l = at + i
            both = dot(stacked(days, -DAY_HALF, i), before[l]) + dot(
                stacked(days, days, i), after[l]
            )
            anomaly[l + half] = dot(own_band, own[l]) + both[:days]
            anomaly[last + half] = anomaly[last + half] + both[PAD : PAD + days]

    def edge(n):
        at, size = order[n]
        low = n % 2 == 0
        if low:
            size = min(size, half - at)
            place = at + lons + half
        else:
            end = at + size
            at = max(at, lons - half)
            size = end - at
            place = at - lons + half
        side = 0 if low else 1
        copy = pltpu.make_async_remote_copy(
            src_ref=anomaly.at[pl.ds(at + half, size)],
            dst_ref=anomaly.at[pl.ds(place, size)],
            send_sem=lon_send.at[side, n],
            recv_sem=lon_recv.at[side, n],
            device_id={"lon": lon_back if low else lon_next},
            device_id_type=MESH,
        )
        copy.start()
        return copy

    for n in range(LEAD):
        whole(n)
    for n in range(len(order)):
        pack(n)
        if n > 0:
            packed(n - 1)
        if n + LEAD < len(order):
            whole(n + LEAD)

    packed(len(order) - 1)

    shifts = []
    for n in range(len(edges)):
        daily(n)
        if n > 0:
            shifts.append(edge(n - 1))

    scale = 1.0 / ((2 * DAY_HALF + 1) * (2 * half + 1))
    width = 2 * half + 1

    def up_to(lo, hi, total):
        def step(l, total):
            total = total + (anomaly[l + width - 1] - anomaly[l - 1])
            out[l] = total * scale
            return total

        return lax.fori_loop(lo, hi, step, total)

    def back(step, total):
        l = half - 1 - step
        total = total + (anomaly[l] - anomaly[l + width])
        out[l] = total * scale
        return total

    total = None
    done = half
    for n in range(len(edges), len(order)):
        end = n == len(order) - 1
        if end and total is not None:
            for copy in shifts:
                copy.wait_recv()
            lax.fori_loop(0, half, back, first)
        daily(n)
        if n == len(edges):
            shifts.append(edge(n - 1))
        ready = lons - half if end else sum(order[n]) - half
        if ready <= half:
            continue
        fresh = total is None
        if fresh:
            total = lax.fori_loop(
                half,
                half + width,
                lambda l, t: t + anomaly[l],
                jnp.zeros((days, cols), jnp.float32),
            )
            out[half] = total * scale
            first = total
            done = half + 1
        total = up_to(done, ready, total)
        done = ready
    up_to(done, lons, total)

    for copies in swaps:
        for copy in copies:
            copy.wait_send()
    for copy in shifts:
        copy.wait_send()


def local(counts, field):
    days, lons, cols = field.shape
    x = jnp.transpose(field, (1, 0, 2))
    edges, middle = plan(lons)
    steps = len(edges) + len(middle)
    rest = middle[-1][1]
    y = pl.pallas_call(
        functools.partial(kernel, counts),
        out_shape=pltpu.VMEM((lons, days, cols), jnp.float32),
        in_specs=[pl.BlockSpec(memory_space=pltpu.HBM)],
        out_specs=pl.BlockSpec(memory_space=pltpu.VMEM),
        scratch_shapes=[
            pltpu.VMEM((lons, days, cols), jnp.bfloat16),
            pltpu.VMEM((lons, 2 * ROWS, cols), jnp.bfloat16),
            pltpu.VMEM((lons, 2 * ROWS, cols), jnp.bfloat16),
            pltpu.VMEM((rest, DAY_HALF, cols), jnp.bfloat16),
            pltpu.VMEM((rest, 2 * ROWS, cols), jnp.bfloat16),
            pltpu.VMEM((lons, ROWS, cols), jnp.bfloat16),
            pltpu.VMEM((lons, ROWS, cols), jnp.bfloat16),
            pltpu.VMEM((lons + 2 * LON_HALF, days, cols), jnp.float32),
            pltpu.SemaphoreType.DMA((steps,)),
            pltpu.SemaphoreType.DMA((2, 2, steps)),
            pltpu.SemaphoreType.DMA((2, 2, steps)),
            pltpu.SemaphoreType.DMA((2, len(edges))),
            pltpu.SemaphoreType.DMA((2, len(edges))),
        ],
        compiler_params=pltpu.CompilerParams(
            collective_id=0, has_side_effects=True, vmem_limit_bytes=50 * 1024 * 1024
        ),
    )(x)
    return jnp.transpose(y, (1, 0, 2))


def solution(mesh):
    return jax.shard_map(
        functools.partial(local, (mesh.shape["day"], mesh.shape["lon"])),
        mesh=mesh,
        in_specs=(P("day", "lon", None),),
        out_specs=P("day", "lon", None),
        check_vma=False,
    )
```

```python
import functools

import jax
import jax.numpy as jnp
from jax import lax
from jax.experimental import pallas as pl
from jax.experimental.pallas import tpu as pltpu
from jax.sharding import PartitionSpec as P

DAY_HALF = 15
LON_HALF = 10
ROWS = 8
PAD = 24
LEAD = 3
MESH = pl.DeviceIdType.MESH


def plan(lons):
    group = DAY_HALF % ROWS + 1
    depth = -(-LON_HALF // group) * group
    left = [(at, group) for at in range(0, depth, group)]
    right = [(lons - at - group, group) for at in range(0, depth, group)]
    edges = [piece for pair in zip(left, right) for piece in pair]
    middle = [
        (at, min(group, lons - depth - at)) for at in range(depth, lons - depth, group)
    ]
    return edges, middle


def grid(rows, cols):
    return (
        lax.broadcasted_iota(jnp.int32, (rows, cols), 0),
        lax.broadcasted_iota(jnp.int32, (rows, cols), 1),
    )


def ones(condition):
    return jnp.where(condition, 1.0, 0.0).astype(jnp.bfloat16)


def band(days, rows, shift):
    day, other = grid(days, rows)
    away = jnp.abs(day - other - shift)
    weight = jnp.where(away <= DAY_HALF, -1.0, 0.0)
    if shift == 0:
        weight = jnp.where(away == 0, 2.0 * DAY_HALF, weight)
    return weight.astype(jnp.bfloat16)


def stacked(days, shift, extra):
    row, other = grid(2 * PAD, 2 * ROWS)
    low = (row < days) & (other < DAY_HALF) & (jnp.abs(row - other - shift) <= DAY_HALF)
    away = jnp.abs(row - PAD - (ROWS + extra) - shift)
    high = (row >= PAD) & (row < PAD + days) & (other == DAY_HALF) & (away <= DAY_HALF)
    return jnp.where(low | high, -1.0, 0.0).astype(jnp.bfloat16)


def kernel(
    counts, x, out, own, before, after, rest_before, rest_after, pack_up, pack_down,
    anomaly, own_sem, day_send, day_recv, lon_send, lon_recv,
):
    lons, days, cols = x.shape
    half = LON_HALF
    tail = days - DAY_HALF
    part = DAY_HALF - ROWS
    group = part + 1
    day_count, lon_count = counts
    day, lon = lax.axis_index("day"), lax.axis_index("lon")
    day_next = lax.rem(day + 1, day_count)
    day_back = lax.rem(day + day_count - 1, day_count)
    lon_next = lax.rem(lon + 1, lon_count)
    lon_back = lax.rem(lon + lon_count - 1, lon_count)
    edges, middle = plan(lons)
    order = edges + middle

    loads = []
    for n, (at, size) in enumerate(order):
        loads.append(
            pltpu.make_async_copy(
                x.at[pl.ds(at, size)], own.at[pl.ds(at, size)], own_sem.at[n]
            )
        )
        loads[-1].start()

    barrier = pltpu.get_barrier_semaphore()
    for axis, peer in (
        ("day", day_next), ("day", day_back), ("lon", lon_next), ("lon", lon_back),
    ):
        pl.semaphore_signal(
            barrier, inc=1, device_id={axis: peer}, device_id_type=MESH
        )
    pl.semaphore_wait(barrier, 4)

    swaps = [[] for _ in order]

    def swap(n, kind, up_src, up_dst, down_src, down_dst):
        for way, src, dst, peer in (
            (0, up_src, up_dst, day_next), (1, down_src, down_dst, day_back),
        ):
            copy = pltpu.make_async_remote_copy(
                src_ref=src,
                dst_ref=dst,
                send_sem=day_send.at[kind, way, n],
                recv_sem=day_recv.at[kind, way, n],
                device_id={"day": peer},
                device_id_type=MESH,
            )
            copy.start()
            swaps[n].append(copy)

    def whole(n):
        at, size = order[n]
        if size == group:
            rows = pl.ds(at, size)
            swap(
                n, 0,
                x.at[rows, pl.ds(tail, ROWS)], before.at[rows, pl.ds(0, ROWS)],
                x.at[rows, pl.ds(0, ROWS)], after.at[rows, pl.ds(0, ROWS)],
            )
        else:
            rows = pl.ds(at, size)
            swap(
                n, 0,
                x.at[rows, pl.ds(tail, DAY_HALF)], rest_before,
                x.at[rows, pl.ds(0, 2 * ROWS)], rest_after,
            )

    row, col = grid(2 * ROWS, days)
    first_day = jnp.where(row < ROWS, tail + ROWS, ROWS)
    place = jnp.where(row < ROWS, row, row - ROWS)
    keep = ones((place < part) & (col == first_day + place))

    def dot(weight, values):
        return jnp.dot(weight, values, preferred_element_type=jnp.float32)

    def pack(n):
        at, size = order[n]
        loads[n].wait()
        if size < group:
            return

        @pl.loop(0, part)
        def _(i):
            ride = ones((place == part) & (col == first_day + i))
            tile = dot(keep, own[at + i]) + dot(ride, own[at + part])
            tile = tile.astype(jnp.bfloat16)
            pack_up[at + i] = tile[:ROWS]
            pack_down[at + i] = tile[ROWS:]

    def packed(n):
        at, size = order[n]
        if size == group:
            rows = pl.ds(at, part)
            swap(
                n, 1,
                pack_up.at[rows], before.at[rows, pl.ds(ROWS, ROWS)],
                pack_down.at[rows], after.at[rows, pl.ds(ROWS, ROWS)],
            )

    own_band = band(days, days, 0)
    before_band = band(days, DAY_HALF, -DAY_HALF)
    after_band = band(days, 2 * ROWS, days)
    before_top = band(days, ROWS, -DAY_HALF)
    after_top = band(days, ROWS, days)

    def daily(n):
        at, size = order[n]
        for copy in swaps[n]:
            copy.wait_recv()
        if size < group:
            for i in range(size):
                anomaly[at + i + half] = (
                    dot(own_band, own[at + i])
                    + dot(before_band, rest_before[i])
                    + dot(after_band, rest_after[i])
                )
            return

        last = at + part
        anomaly[last + half] = (
            dot(own_band, own[last])
            + dot(before_top, before[last, pl.ds(0, ROWS)])
            + dot(after_top, after[last, pl.ds(0, ROWS)])
        )

        @pl.loop(0, part)
        def _(i):
            l = at + i
            both = dot(stacked(days, -DAY_HALF, i), before[l]) + dot(
                stacked(days, days, i), after[l]
            )
            anomaly[l + half] = dot(own_band, own[l]) + both[:days]
            anomaly[last + half] = anomaly[last + half] + both[PAD : PAD + days]

    def edge(n):
        at, size = order[n]
        low = n % 2 == 0
        if low:
            size = min(size, half - at)
            place = at + lons + half
        else:
            end = at + size
            at = max(at, lons - half)
            size = end - at
            place = at - lons + half
        side = 0 if low else 1
        copy = pltpu.make_async_remote_copy(
            src_ref=anomaly.at[pl.ds(at + half, size)],
            dst_ref=anomaly.at[pl.ds(place, size)],
            send_sem=lon_send.at[side, n],
            recv_sem=lon_recv.at[side, n],
            device_id={"lon": lon_back if low else lon_next},
            device_id_type=MESH,
        )
        copy.start()
        return copy

    steps = len(order)
    for n in range(LEAD):
        whole(n)
    for n in range(LEAD):
        pack(n)
        if n > 0:
            packed(n - 1)

    shifts = []

    def advance(n):
        daily(n)
        if n + LEAD < steps:
            pack(n + LEAD)
        if n < len(edges):
            shifts.append(edge(n))
        if n + LEAD - 1 < steps:
            packed(n + LEAD - 1)
        if n + LEAD < steps:
            whole(n + LEAD)

    for n in range(len(edges)):
        advance(n)

    scale = 1.0 / ((2 * DAY_HALF + 1) * (2 * half + 1))
    width = 2 * half + 1

    def up_to(lo, hi, total):
        def step(l, total):
            total = total + (anomaly[l + width - 1] - anomaly[l - 1])
            out[l] = total * scale
            return total

        return lax.fori_loop(lo, hi, step, total)

    def back(step, total):
        l = half - 1 - step
        total = total + (anomaly[l] - anomaly[l + width])
        out[l] = total * scale
        return total

    total = None
    done = half
    for n in range(len(edges), steps):
        end = n == steps - 1
        if end and total is not None:
            for copy in shifts:
                copy.wait_recv()
            lax.fori_loop(0, half, back, first)
        advance(n)
        ready = lons - half if end else sum(order[n]) - half
        if ready <= half:
            continue
        fresh = total is None
        if fresh:
            total = lax.fori_loop(
                half,
                half + width,
                lambda l, t: t + anomaly[l],
                jnp.zeros((days, cols), jnp.float32),
            )
            out[half] = total * scale
            first = total
            done = half + 1
        total = up_to(done, ready, total)
        done = ready
    up_to(done, lons, total)

    for copies in swaps:
        for copy in copies:
            copy.wait_send()
    for copy in shifts:
        copy.wait_send()


def local(counts, field):
    days, lons, cols = field.shape
    x = jnp.transpose(field, (1, 0, 2))
    edges, middle = plan(lons)
    steps = len(edges) + len(middle)
    rest = middle[-1][1]
    y = pl.pallas_call(
        functools.partial(kernel, counts),
        out_shape=pltpu.VMEM((lons, days, cols), jnp.float32),
        in_specs=[pl.BlockSpec(memory_space=pltpu.HBM)],
        out_specs=pl.BlockSpec(memory_space=pltpu.VMEM),
        scratch_shapes=[
            pltpu.VMEM((lons, days, cols), jnp.bfloat16),
            pltpu.VMEM((lons, 2 * ROWS, cols), jnp.bfloat16),
            pltpu.VMEM((lons, 2 * ROWS, cols), jnp.bfloat16),
            pltpu.VMEM((rest, DAY_HALF, cols), jnp.bfloat16),
            pltpu.VMEM((rest, 2 * ROWS, cols), jnp.bfloat16),
            pltpu.VMEM((lons, ROWS, cols), jnp.bfloat16),
            pltpu.VMEM((lons, ROWS, cols), jnp.bfloat16),
            pltpu.VMEM((lons + 2 * LON_HALF, days, cols), jnp.float32),
            pltpu.SemaphoreType.DMA((steps,)),
            pltpu.SemaphoreType.DMA((2, 2, steps)),
            pltpu.SemaphoreType.DMA((2, 2, steps)),
            pltpu.SemaphoreType.DMA((2, len(edges))),
            pltpu.SemaphoreType.DMA((2, len(edges))),
        ],
        compiler_params=pltpu.CompilerParams(
            collective_id=0, has_side_effects=True, vmem_limit_bytes=50 * 1024 * 1024
        ),
    )(x)
    return jnp.transpose(y, (1, 0, 2))


def solution(mesh):
    return jax.shard_map(
        functools.partial(local, (mesh.shape["day"], mesh.shape["lon"])),
        mesh=mesh,
        in_specs=(P("day", "lon", None),),
        out_specs=P("day", "lon", None),
        check_vma=False,
    )
```

```python
import functools

import jax
import jax.numpy as jnp
from jax import lax
from jax.experimental import pallas as pl
from jax.experimental.pallas import tpu as pltpu
from jax.sharding import PartitionSpec as P

DAY_HALF = 15
LON_HALF = 10
ROWS = 8
PAD = 24
LEAD = 3
MESH = pl.DeviceIdType.MESH


def plan(lons):
    group = DAY_HALF % ROWS + 1
    depth = -(-LON_HALF // group) * group
    left = [(at, group) for at in range(0, depth, group)]
    right = [(lons - at - group, group) for at in range(0, depth, group)]
    edges = [piece for pair in zip(left, right) for piece in pair]
    middle = [
        (at, min(group, lons - depth - at)) for at in range(depth, lons - depth, group)
    ]
    return edges, middle


def grid(rows, cols):
    return (
        lax.broadcasted_iota(jnp.int32, (rows, cols), 0),
        lax.broadcasted_iota(jnp.int32, (rows, cols), 1),
    )


def ones(condition):
    return jnp.where(condition, 1.0, 0.0).astype(jnp.bfloat16)


def band(days, rows, shift):
    day, other = grid(days, rows)
    away = jnp.abs(day - other - shift)
    weight = jnp.where(away <= DAY_HALF, -1.0, 0.0)
    if shift == 0:
        weight = jnp.where(away == 0, 2.0 * DAY_HALF, weight)
    return weight.astype(jnp.bfloat16)


def stacked(days, shift, extra):
    row, other = grid(2 * PAD, 2 * ROWS)
    low = (row < days) & (other < DAY_HALF) & (jnp.abs(row - other - shift) <= DAY_HALF)
    away = jnp.abs(row - PAD - (ROWS + extra) - shift)
    high = (row >= PAD) & (row < PAD + days) & (other == DAY_HALF) & (away <= DAY_HALF)
    return jnp.where(low | high, -1.0, 0.0).astype(jnp.bfloat16)


def kernel(
    counts, x, out, own, before, after, rest_before, rest_after, pack_up, pack_down,
    anomaly, own_sem, day_send, day_recv, lon_send, lon_recv,
    day_ready, lon_ready,
):
    lons, days, cols = x.shape
    half = LON_HALF
    tail = days - DAY_HALF
    part = DAY_HALF - ROWS
    group = part + 1
    day_count, lon_count = counts
    day, lon = lax.axis_index("day"), lax.axis_index("lon")
    day_next = lax.rem(day + 1, day_count)
    day_back = lax.rem(day + day_count - 1, day_count)
    lon_next = lax.rem(lon + 1, lon_count)
    lon_back = lax.rem(lon + lon_count - 1, lon_count)
    edges, middle = plan(lons)
    order = edges + middle

    loads = []
    for n, (at, size) in enumerate(order):
        loads.append(
            pltpu.make_async_copy(
                x.at[pl.ds(at, size)], own.at[pl.ds(at, size)], own_sem.at[n]
            )
        )
        loads[-1].start()

    barrier = pltpu.get_barrier_semaphore()
    even = lax.rem(day, 2) == 0
    odd = jnp.logical_not(even)

    def tell(semaphore, axis, peers):
        for peer in peers:
            pl.semaphore_signal(
                semaphore, inc=1, device_id={axis: peer}, device_id_type=MESH
            )

    @pl.when(odd)
    def _():
        tell(barrier, "day", (day_next, day_back))

    @pl.when(even)
    def _():
        pl.semaphore_wait(barrier, 2)
        tell(day_ready, "day", (day_next, day_back))

    @pl.when(odd)
    def _():
        pl.semaphore_wait(day_ready, 2)
        tell(barrier, "lon", (lon_next, lon_back))

    swaps = [[] for _ in order]

    def swap(n, kind, up_src, up_dst, down_src, down_dst):
        for way, src, dst, peer in (
            (0, up_src, up_dst, day_next), (1, down_src, down_dst, day_back),
        ):
            copy = pltpu.make_async_remote_copy(
                src_ref=src,
                dst_ref=dst,
                send_sem=day_send.at[kind, way, n],
                recv_sem=day_recv.at[kind, way, n],
                device_id={"day": peer},
                device_id_type=MESH,
            )
            copy.start()
            swaps[n].append(copy)

    def whole(n):
        at, size = order[n]
        if size == group:
            rows = pl.ds(at, size)
            swap(
                n, 0,
                x.at[rows, pl.ds(tail, ROWS)], before.at[rows, pl.ds(0, ROWS)],
                x.at[rows, pl.ds(0, ROWS)], after.at[rows, pl.ds(0, ROWS)],
            )
        else:
            rows = pl.ds(at, size)
            swap(
                n, 0,
                x.at[rows, pl.ds(tail, DAY_HALF)], rest_before,
                x.at[rows, pl.ds(0, 2 * ROWS)], rest_after,
            )

    row, col = grid(2 * ROWS, days)
    first_day = jnp.where(row < ROWS, tail + ROWS, ROWS)
    place = jnp.where(row < ROWS, row, row - ROWS)
    keep = ones((place < part) & (col == first_day + place))

    def dot(weight, values):
        return jnp.dot(weight, values, preferred_element_type=jnp.float32)

    def pack(n):
        at, size = order[n]
        loads[n].wait()
        if size < group:
            return

        @pl.loop(0, part)
        def _(i):
            ride = ones((place == part) & (col == first_day + i))
            tile = dot(keep, own[at + i]) + dot(ride, own[at + part])
            tile = tile.astype(jnp.bfloat16)
            pack_up[at + i] = tile[:ROWS]
            pack_down[at + i] = tile[ROWS:]

    def packed(n):
        at, size = order[n]
        if size == group:
            rows = pl.ds(at, part)
            swap(
                n, 1,
                pack_up.at[rows], before.at[rows, pl.ds(ROWS, ROWS)],
                pack_down.at[rows], after.at[rows, pl.ds(ROWS, ROWS)],
            )

    own_band = band(days, days, 0)
    before_band = band(days, DAY_HALF, -DAY_HALF)
    after_band = band(days, 2 * ROWS, days)
    before_top = band(days, ROWS, -DAY_HALF)
    after_top = band(days, ROWS, days)

    def daily(n):
        at, size = order[n]
        for copy in swaps[n]:
            copy.wait_recv()
        if size < group:
            for i in range(size):
                anomaly[at + i + half] = (
                    dot(own_band, own[at + i])
                    + dot(before_band, rest_before[i])
                    + dot(after_band, rest_after[i])
                )
            return

        last = at + part
        anomaly[last + half] = (
            dot(own_band, own[last])
            + dot(before_top, before[last, pl.ds(0, ROWS)])
            + dot(after_top, after[last, pl.ds(0, ROWS)])
        )

        @pl.loop(0, part)
        def _(i):
            l = at + i
            both = dot(stacked(days, -DAY_HALF, i), before[l]) + dot(
                stacked(days, days, i), after[l]
            )
            anomaly[l + half] = dot(own_band, own[l]) + both[:days]
            anomaly[last + half] = anomaly[last + half] + both[PAD : PAD + days]

    def edge(n):
        at, size = order[n]
        low = n % 2 == 0
        if low:
            size = min(size, half - at)
            place = at + lons + half
        else:
            end = at + size
            at = max(at, lons - half)
            size = end - at
            place = at - lons + half
        side = 0 if low else 1
        copy = pltpu.make_async_remote_copy(
            src_ref=anomaly.at[pl.ds(at + half, size)],
            dst_ref=anomaly.at[pl.ds(place, size)],
            send_sem=lon_send.at[side, n],
            recv_sem=lon_recv.at[side, n],
            device_id={"lon": lon_back if low else lon_next},
            device_id_type=MESH,
        )
        copy.start()
        return copy

    steps = len(order)
    for n in range(LEAD):
        whole(n)
    for n in range(steps):
        pack(n)
        if n > 0:
            packed(n - 1)
    packed(steps - 1)
    for n in range(LEAD, steps):
        whole(n)
    shifts = []

    def advance(n):
        daily(n)
        if 0 < n <= len(edges):
            shifts.append(edge(n - 1))

    @pl.when(odd)
    def _():
        pl.semaphore_wait(barrier, 2)
        tell(lon_ready, "day", (day_back,))

    @pl.when(even)
    def _():
        pl.semaphore_wait(lon_ready, 1)

    for n in range(len(edges)):
        advance(n)

    scale = 1.0 / ((2 * DAY_HALF + 1) * (2 * half + 1))
    width = 2 * half + 1

    def up_to(lo, hi, total):
        def step(l, total):
            total = total + (anomaly[l + width - 1] - anomaly[l - 1])
            out[l] = total * scale
            return total

        return lax.fori_loop(lo, hi, step, total)

    def back(step, total):
        l = half - 1 - step
        total = total + (anomaly[l] - anomaly[l + width])
        out[l] = total * scale
        return total

    total = None
    done = half
    for n in range(len(edges), steps):
        end = n == steps - 1
        if end and total is not None:
            for copy in shifts:
                copy.wait_recv()
            lax.fori_loop(0, half, back, first)
        advance(n)
        ready = lons - half if end else sum(order[n]) - half
        if ready <= half:
            continue
        fresh = total is None
        if fresh:
            total = lax.fori_loop(
                half,
                half + width,
                lambda l, t: t + anomaly[l],
                jnp.zeros((days, cols), jnp.float32),
            )
            out[half] = total * scale
            first = total
            done = half + 1
        total = up_to(done, ready, total)
        done = ready
    up_to(done, lons, total)

    for copies in swaps:
        for copy in copies:
            copy.wait_send()
    for copy in shifts:
        copy.wait_send()


def local(counts, field):
    days, lons, cols = field.shape
    x = jnp.transpose(field, (1, 0, 2))
    edges, middle = plan(lons)
    steps = len(edges) + len(middle)
    rest = middle[-1][1]
    y = pl.pallas_call(
        functools.partial(kernel, counts),
        out_shape=pltpu.VMEM((lons, days, cols), jnp.float32),
        in_specs=[pl.BlockSpec(memory_space=pltpu.HBM)],
        out_specs=pl.BlockSpec(memory_space=pltpu.VMEM),
        scratch_shapes=[
            pltpu.VMEM((lons, days, cols), jnp.bfloat16),
            pltpu.VMEM((lons, 2 * ROWS, cols), jnp.bfloat16),
            pltpu.VMEM((lons, 2 * ROWS, cols), jnp.bfloat16),
            pltpu.VMEM((rest, DAY_HALF, cols), jnp.bfloat16),
            pltpu.VMEM((rest, 2 * ROWS, cols), jnp.bfloat16),
            pltpu.VMEM((lons, ROWS, cols), jnp.bfloat16),
            pltpu.VMEM((lons, ROWS, cols), jnp.bfloat16),
            pltpu.VMEM((lons + 2 * LON_HALF, days, cols), jnp.float32),
            pltpu.SemaphoreType.DMA((steps,)),
            pltpu.SemaphoreType.DMA((2, 2, steps)),
            pltpu.SemaphoreType.DMA((2, 2, steps)),
            pltpu.SemaphoreType.DMA((2, len(edges))),
            pltpu.SemaphoreType.DMA((2, len(edges))),
            pltpu.SemaphoreType.REGULAR,
            pltpu.SemaphoreType.REGULAR,
        ],
        compiler_params=pltpu.CompilerParams(
            collective_id=0, has_side_effects=True, vmem_limit_bytes=50 * 1024 * 1024
        ),
    )(x)
    return jnp.transpose(y, (1, 0, 2))


def solution(mesh):
    return jax.shard_map(
        functools.partial(local, (mesh.shape["day"], mesh.shape["lon"])),
        mesh=mesh,
        in_specs=(P("day", "lon", None),),
        out_specs=P("day", "lon", None),
        check_vma=False,
    )
```

```python
import functools

import jax
import jax.numpy as jnp
from jax import lax
from jax.experimental import pallas as pl
from jax.experimental.pallas import tpu as pltpu
from jax.sharding import PartitionSpec as P

DAY_HALF = 15
LON_HALF = 10
ROWS = 8
PAD = 24
LEAD = 2
MESH = pl.DeviceIdType.MESH


def plan(lons):
    group = DAY_HALF % ROWS + 1
    depth = -(-LON_HALF // group) * group
    left = [(at, group) for at in range(0, depth, group)]
    right = [(lons - at - group, group) for at in range(0, depth, group)]
    edges = [piece for pair in zip(left, right) for piece in pair]
    middle = [
        (at, min(group, lons - depth - at)) for at in range(depth, lons - depth, group)
    ]
    return edges, middle


def grid(rows, cols):
    return (
        lax.broadcasted_iota(jnp.int32, (rows, cols), 0),
        lax.broadcasted_iota(jnp.int32, (rows, cols), 1),
    )


def ones(condition):
    return jnp.where(condition, 1.0, 0.0).astype(jnp.bfloat16)


def band(days, rows, shift):
    day, other = grid(days, rows)
    away = jnp.abs(day - other - shift)
    weight = jnp.where(away <= DAY_HALF, -1.0, 0.0)
    if shift == 0:
        weight = jnp.where(away == 0, 2.0 * DAY_HALF, weight)
    return weight.astype(jnp.bfloat16)


def stacked(days, shift, extra):
    row, other = grid(2 * PAD, 2 * ROWS)
    low = (row < days) & (other < DAY_HALF) & (jnp.abs(row - other - shift) <= DAY_HALF)
    away = jnp.abs(row - PAD - (ROWS + extra) - shift)
    high = (row >= PAD) & (row < PAD + days) & (other == DAY_HALF) & (away <= DAY_HALF)
    return jnp.where(low | high, -1.0, 0.0).astype(jnp.bfloat16)


def kernel(
    counts, x, out, own, before, after, rest_before, rest_after, pack_up, pack_down,
    anomaly, own_sem, day_send, day_recv, lon_send, lon_recv,
    day_ready, lon_ready,
):
    lons, days, cols = x.shape
    half = LON_HALF
    tail = days - DAY_HALF
    part = DAY_HALF - ROWS
    group = part + 1
    day_count, lon_count = counts
    day, lon = lax.axis_index("day"), lax.axis_index("lon")
    day_next = lax.rem(day + 1, day_count)
    day_back = lax.rem(day + day_count - 1, day_count)
    lon_next = lax.rem(lon + 1, lon_count)
    lon_back = lax.rem(lon + lon_count - 1, lon_count)
    edges, middle = plan(lons)
    order = edges + middle

    loads = []
    for n, (at, size) in enumerate(order):
        loads.append(
            pltpu.make_async_copy(
                x.at[pl.ds(at, size)], own.at[pl.ds(at, size)], own_sem.at[n]
            )
        )
        loads[-1].start()

    barrier = pltpu.get_barrier_semaphore()
    even = lax.rem(day, 2) == 0
    odd = jnp.logical_not(even)

    def tell(semaphore, axis, peers):
        for peer in peers:
            pl.semaphore_signal(
                semaphore, inc=1, device_id={axis: peer}, device_id_type=MESH
            )

    @pl.when(odd)
    def _():
        tell(barrier, "day", (day_next, day_back))

    @pl.when(even)
    def _():
        pl.semaphore_wait(barrier, 2)
        tell(day_ready, "day", (day_next, day_back))

    @pl.when(odd)
    def _():
        pl.semaphore_wait(day_ready, 2)
        tell(barrier, "lon", (lon_next, lon_back))

    swaps = [[] for _ in order]

    def swap(n, kind, up_src, up_dst, down_src, down_dst):
        for way, src, dst, peer in (
            (0, up_src, up_dst, day_next), (1, down_src, down_dst, day_back),
        ):
            copy = pltpu.make_async_remote_copy(
                src_ref=src,
                dst_ref=dst,
                send_sem=day_send.at[kind, way, n],
                recv_sem=day_recv.at[kind, way, n],
                device_id={"day": peer},
                device_id_type=MESH,
            )
            copy.start()
            swaps[n].append(copy)

    def whole(n):
        at, size = order[n]
        if size == group:
            rows = pl.ds(at, size)
            swap(
                n, 0,
                x.at[rows, pl.ds(tail, ROWS)], before.at[rows, pl.ds(0, ROWS)],
                x.at[rows, pl.ds(0, ROWS)], after.at[rows, pl.ds(0, ROWS)],
            )
        else:
            rows = pl.ds(at, size)
            swap(
                n, 0,
                x.at[rows, pl.ds(tail, DAY_HALF)], rest_before,
                x.at[rows, pl.ds(0, 2 * ROWS)], rest_after,
            )

    row, col = grid(2 * ROWS, days)
    first_day = jnp.where(row < ROWS, tail + ROWS, ROWS)
    place = jnp.where(row < ROWS, row, row - ROWS)
    keep = ones((place < part) & (col == first_day + place))

    def dot(weight, values):
        return jnp.dot(weight, values, preferred_element_type=jnp.float32)

    def pack(n):
        at, size = order[n]
        loads[n].wait()
        if size < group:
            return

        @pl.loop(0, part)
        def _(i):
            ride = ones((place == part) & (col == first_day + i))
            tile = dot(keep, own[at + i]) + dot(ride, own[at + part])
            tile = tile.astype(jnp.bfloat16)
            pack_up[at + i] = tile[:ROWS]
            pack_down[at + i] = tile[ROWS:]

    def packed(n):
        at, size = order[n]
        if size == group:
            rows = pl.ds(at, part)
            swap(
                n, 1,
                pack_up.at[rows], before.at[rows, pl.ds(ROWS, ROWS)],
                pack_down.at[rows], after.at[rows, pl.ds(ROWS, ROWS)],
            )

    own_band = band(days, days, 0)
    before_band = band(days, DAY_HALF, -DAY_HALF)
    after_band = band(days, 2 * ROWS, days)
    before_top = band(days, ROWS, -DAY_HALF)
    after_top = band(days, ROWS, days)

    def daily(n):
        at, size = order[n]
        for copy in swaps[n]:
            copy.wait_recv()
        if size < group:
            for i in range(size):
                anomaly[at + i + half] = (
                    dot(own_band, own[at + i])
                    + dot(before_band, rest_before[i])
                    + dot(after_band, rest_after[i])
                )
            return

        last = at + part
        anomaly[last + half] = (
            dot(own_band, own[last])
            + dot(before_top, before[last, pl.ds(0, ROWS)])
            + dot(after_top, after[last, pl.ds(0, ROWS)])
        )

        @pl.loop(0, part)
        def _(i):
            l = at + i
            both = dot(stacked(days, -DAY_HALF, i), before[l]) + dot(
                stacked(days, days, i), after[l]
            )
            anomaly[l + half] = dot(own_band, own[l]) + both[:days]
            anomaly[last + half] = anomaly[last + half] + both[PAD : PAD + days]

    def edge(n):
        at, size = order[n]
        low = n % 2 == 0
        if low:
            size = min(size, half - at)
            place = at + lons + half
        else:
            end = at + size
            at = max(at, lons - half)
            size = end - at
            place = at - lons + half
        side = 0 if low else 1
        copy = pltpu.make_async_remote_copy(
            src_ref=anomaly.at[pl.ds(at + half, size)],
            dst_ref=anomaly.at[pl.ds(place, size)],
            send_sem=lon_send.at[side, n],
            recv_sem=lon_recv.at[side, n],
            device_id={"lon": lon_back if low else lon_next},
            device_id_type=MESH,
        )
        copy.start()
        return copy

    steps = len(order)
    for n in range(LEAD):
        whole(n)
    for n in range(steps):
        pack(n)
        if n > 0:
            packed(n - 1)
    packed(steps - 1)
    for n in range(LEAD, steps):
        whole(n)
    shifts = []

    def advance(n):
        daily(n)
        if 0 < n <= len(edges):
            shifts.append(edge(n - 1))

    @pl.when(odd)
    def _():
        pl.semaphore_wait(barrier, 2)
        tell(lon_ready, "day", (day_back,))

    @pl.when(even)
    def _():
        pl.semaphore_wait(lon_ready, 1)

    for n in range(len(edges)):
        advance(n)

    scale = 1.0 / ((2 * DAY_HALF + 1) * (2 * half + 1))
    width = 2 * half + 1

    def up_to(lo, hi, total):
        def step(l, total):
            total = total + (anomaly[l + width - 1] - anomaly[l - 1])
            out[l] = total * scale
            return total

        return lax.fori_loop(lo, hi, step, total)

    def back(step, total):
        l = half - 1 - step
        total = total + (anomaly[l] - anomaly[l + width])
        out[l] = total * scale
        return total

    total = None
    done = half
    for n in range(len(edges), steps):
        end = n == steps - 1
        if end and total is not None:
            for copy in shifts:
                copy.wait_recv()
            lax.fori_loop(0, half, back, first)
        advance(n)
        ready = lons - half if end else sum(order[n]) - half
        if ready <= half:
            continue
        fresh = total is None
        if fresh:
            total = lax.fori_loop(
                half,
                half + width,
                lambda l, t: t + anomaly[l],
                jnp.zeros((days, cols), jnp.float32),
            )
            out[half] = total * scale
            first = total
            done = half + 1
        total = up_to(done, ready, total)
        done = ready
    up_to(done, lons, total)

    for copies in swaps:
        for copy in copies:
            copy.wait_send()
    for copy in shifts:
        copy.wait_send()


def local(counts, field):
    days, lons, cols = field.shape
    x = jnp.transpose(field, (1, 0, 2))
    edges, middle = plan(lons)
    steps = len(edges) + len(middle)
    rest = middle[-1][1]
    y = pl.pallas_call(
        functools.partial(kernel, counts),
        out_shape=pltpu.VMEM((lons, days, cols), jnp.float32),
        in_specs=[pl.BlockSpec(memory_space=pltpu.HBM)],
        out_specs=pl.BlockSpec(memory_space=pltpu.VMEM),
        scratch_shapes=[
            pltpu.VMEM((lons, days, cols), jnp.bfloat16),
            pltpu.VMEM((lons, 2 * ROWS, cols), jnp.bfloat16),
            pltpu.VMEM((lons, 2 * ROWS, cols), jnp.bfloat16),
            pltpu.VMEM((rest, DAY_HALF, cols), jnp.bfloat16),
            pltpu.VMEM((rest, 2 * ROWS, cols), jnp.bfloat16),
            pltpu.VMEM((lons, ROWS, cols), jnp.bfloat16),
            pltpu.VMEM((lons, ROWS, cols), jnp.bfloat16),
            pltpu.VMEM((lons + 2 * LON_HALF, days, cols), jnp.float32),
            pltpu.SemaphoreType.DMA((steps,)),
            pltpu.SemaphoreType.DMA((2, 2, steps)),
            pltpu.SemaphoreType.DMA((2, 2, steps)),
            pltpu.SemaphoreType.DMA((2, len(edges))),
            pltpu.SemaphoreType.DMA((2, len(edges))),
            pltpu.SemaphoreType.REGULAR,
            pltpu.SemaphoreType.REGULAR,
        ],
        compiler_params=pltpu.CompilerParams(
            collective_id=0, has_side_effects=True, vmem_limit_bytes=50 * 1024 * 1024
        ),
    )(x)
    return jnp.transpose(y, (1, 0, 2))


def solution(mesh):
    return jax.shard_map(
        functools.partial(local, (mesh.shape["day"], mesh.shape["lon"])),
        mesh=mesh,
        in_specs=(P("day", "lon", None),),
        out_specs=P("day", "lon", None),
        check_vma=False,
    )
```
